32 devices in a mesh: group: 2 (over y), member: 16 (over z, x, core).
Axes of the slice: x: 2, y: 2, z: 4, core: 2. Of those that a mesh axis runs over, the one named last changes fastest.
Arguments:
- state: float32 [512, 64, 128], P(('group', 'member')), may hold values from -2.5 to 2.5
- blocks: bfloat16 [512, 6, 128, 128], P(('group', 'member')), may hold values from -1 to 1
- rate: float32 [512, 128], P(('group', 'member')), may hold values from 0.1 to 1
- own_col: int32 [512], P(('group', 'member')), may hold values from 0 to 15
- member_col: int32 [512, 4], P(('group', 'member')), may hold values from 0 to 15, as said below
- group_col: int32 [512, 1], P(('group', 'member')), may hold values from 0 to 3, as said below
- member_send: int32 [32, 16], P(('group', 'member')), may hold values from 0 to 15
- group_send: int32 [32, 4], P(('group', 'member')), may hold values from 0 to 15
Outputs:
- new_state: float32 [512, 64, 128], P(('group', 'member'))
The draws below stay inside these ranges and needn't reach their ends.
Inputs may be any that keep to these rules, and one draw needn't show every extreme that they name: `member_col`: on each device the 64 entries of its rows name every member index equally often. `group_col`: on each device the 16 entries of its rows name every slot equally often.
All inputs are finite; a program needn't handle non-finite values.
Results may differ from the reference program's by a relative error of at most 0.00092.
Values may be sent and summed in bfloat16 or wider, within the bound.
No kernel may reach another device: no remote copies, remote signals or barrier semaphores. Data moves between devices by JAX's collectives and lax.ppermute only.
A program may use at most 64 MiB of HBM per device.

```python
import math
import jax
import jax.numpy as jnp
from jax import lax

CELLS = 128
TRAJ = 64
BR = 16
KM = 4
KG = 1
GG = 2
STEPS = 2
K = 6
MSLOTS = 16
GSLOTS = 4
NB = 512
DEVICES = 32


def spread_slots(key, count, slots):
    keys = jax.random.split(key, DEVICES)
    perms = jax.vmap(lambda one: jax.random.permutation(one, BR * count))(keys)
    return (perms % slots).reshape(DEVICES * BR, count).astype(jnp.int32)


def draw_member_col(key, part):
    return spread_slots(jax.random.fold_in(key, 11), KM, MSLOTS)


def draw_group_col(key, part):
    return spread_slots(jax.random.fold_in(key, 23), KG, GSLOTS)


def place_ends(values, key, low, top_value):
    spot = [jax.random.randint(jax.random.fold_in(key, axis), (), 0, length) for axis, length in enumerate(values.shape)]
    main_axis = values.shape.index(max(values.shape))
    next_to = spot[:main_axis] + [(spot[main_axis] + 1) % values.shape[main_axis]] + spot[main_axis + 1:]
    return values.at[tuple(spot)].set(low).at[tuple(next_to)].set(top_value)


def steps_of(key, extent, cuts, least, top_value):
    level = 1.0
    for axis_at, shards_of in cuts:
        heights = jax.random.uniform(jax.random.fold_in(jax.random.fold_in(key, 6), axis_at), (shards_of,), jnp.float32, least / len(cuts), top_value / len(cuts))
        level = level * jnp.repeat(jnp.exp(heights), extent[axis_at] // shards_of).reshape((-1,) + (1,) * (len(extent) - 1 - axis_at))
    return level


def centred(key, shape, deviation, limit, shards=(), kind=jnp.bfloat16):
    values = deviation * jax.random.normal(key, shape, jnp.float32)
    if shards:
        values = values * steps_of(key, shape, shards, -0.22, 0.18)
    return jnp.clip(values, -limit, limit).astype(kind)


def setup_inputs(seed: int = 0) -> dict:
    key_list = jax.random.split(jax.random.key(seed), 9)
    state = centred(key_list[0], (NB, TRAJ, CELLS), 0.6, 2.5, ((0, 32),), jnp.float32)
    blocks = centred(key_list[1], (NB, K, CELLS, CELLS), (CELLS // 4) ** -0.5, 1.0, ((0, 32),))
    rate = jnp.clip(jnp.exp(math.log(1.0) - 2.3025851 * jax.random.uniform(key_list[2], (NB, CELLS), jnp.float32) ** steps_of(key_list[2], (NB, CELLS), ((0, 32),), -0.2, 0.2)), 0.1, 1.0)
    own_col = place_ends(jax.random.randint(key_list[3], (NB,), 0, BR), jax.random.fold_in(key_list[3], 1), 0, BR - 1).astype(jnp.int32)
    member_col = draw_member_col(jax.random.fold_in(key_list[8], 71), 0)
    group_col = draw_group_col(jax.random.fold_in(key_list[8], 71), 0)
    member_send = place_ends(jax.random.randint(key_list[6], (DEVICES, MSLOTS), 0, BR), jax.random.fold_in(key_list[6], 1), 0, BR - 1).astype(jnp.int32)
    group_send = place_ends(jax.random.randint(key_list[7], (DEVICES, GSLOTS), 0, BR), jax.random.fold_in(key_list[7], 1), 0, BR - 1).astype(jnp.int32)
    return {"state": state, "blocks": blocks, "rate": rate, "own_col": own_col, "member_col": member_col, "group_col": group_col, "member_send": member_send, "group_send": group_send}


step_size = 0.1


def sources(own_col, member_col, group_col, member_send, group_send):
    rows = jnp.arange(NB, dtype=jnp.int32)
    device = rows // BR
    grp = device // MSLOTS
    mem = device % MSLOTS
    own_src = device * BR + own_col
    peer_dev = grp[:, None] * MSLOTS + member_col
    member_src = peer_dev * BR + member_send[peer_dev, mem[:, None]]
    hgroup = group_col // GG
    within = group_col % GG
    far_dev = hgroup * MSLOTS + mem[:, None]
    group_src = far_dev * BR + group_send[far_dev, grp[:, None] * GG + within]
    return jnp.concatenate([own_src[:, None], member_src, group_src], axis=1).astype(jnp.int32)


def derivative(field, blocks, rate, src):
    rounded = field.astype(jnp.bfloat16)

    def one_device(device):
        start = (device * BR).astype(jnp.int32)
        index = lax.dynamic_slice_in_dim(src, start, BR, 0)
        taken = rounded[index].astype(jnp.float32)
        weights = lax.dynamic_slice_in_dim(blocks, start, BR, 0).astype(jnp.float32)
        return jnp.einsum('iktc,ikcd->itd', taken, weights, precision=lax.Precision.HIGHEST)

    product = lax.map(one_device, jnp.arange(DEVICES, dtype=jnp.int32))
    product = product.reshape(NB, TRAJ, CELLS)
    return -product + rate[:, None, :] * (field - field * field * field)


def reference(state, blocks, rate, own_col, member_col, group_col, member_send, group_send):
    src = sources(own_col, member_col, group_col, member_send, group_send)
    current = state
    for step in range(STEPS):
        first = derivative(current, blocks, rate, src)
        second = derivative(current + 0.5 * step_size * first, blocks, rate, src)
        third = derivative(current + 0.5 * step_size * second, blocks, rate, src)
        fourth = derivative(current + step_size * third, blocks, rate, src)
        current = current + (step_size / 6.0) * (first + 2.0 * second + 2.0 * third + fourth)
    return current
```

```python
import functools

import jax
import jax.numpy as jnp
from jax import lax
from jax.experimental import pallas as pl
from jax.experimental.pallas import tpu as pltpu
from jax.sharding import PartitionSpec as P

STEPS = 2
PIECES = 1
VMEM_LIMIT = 16 * 2**20


step_size = 0.1

VMEM = pl.BlockSpec(memory_space=pltpu.VMEM)
SMEM = pl.BlockSpec(memory_space=pltpu.SMEM)


class Sizes:
    def __init__(self, mesh, state, member_col, group_col, member_send, group_send):
        self.groups = mesh.shape["group"]
        self.members = mesh.shape["member"]
        self.rows, self.traj, self.cells = state.shape
        self.near = member_col.shape[1]
        self.far = group_col.shape[1]
        self.sent = group_send.shape[1] // self.groups
        self.piece = self.traj // PIECES
        self.at_own = 0
        self.at_near = self.at_own + self.rows
        self.at_far = self.at_near + self.rows * self.near
        self.at_msend = self.at_far + self.rows * self.far
        self.at_gsend = self.at_msend + self.members
        self.at_group = self.at_gsend + self.groups * self.sent


def group_row(sz, table, shift, slot):
    target = lax.rem(table[sz.at_group] + shift, sz.groups)
    return table[sz.at_gsend + target * sz.sent + slot]


def fill_sends(sz, table, rounded, member_out, group_out):
    for p in range(sz.members):
        member_out[p] = rounded[table[sz.at_msend + p]]
    for shift in range(1, sz.groups):
        for slot in range(sz.sent):
            group_out[(shift - 1) * sz.sent + slot] = rounded[group_row(sz, table, shift, slot)]


def first_kernel(sz, piece, table, state, rounded, member_out, group_out):
    span = pl.ds(piece * sz.piece, sz.piece)
    for i in range(sz.rows):
        rounded[i] = state[i, span].astype(jnp.bfloat16)
    fill_sends(sz, table, rounded, member_out, group_out)


def stage_kernel(sz, stage, last, base_span, *refs):
    it = iter(refs)
    table, blocks, rate, rounded, near, far = (next(it) for _ in range(6))
    base = next(it) if stage < 3 else None
    value = next(it) if stage > 0 else None
    total = next(it) if stage > 0 else None
    if not last:
        rounded_out, member_out, group_out = (next(it) for _ in range(3))
    out = next(it)
    total_out = next(it) if stage < 3 else None
    far_all = next(it)

    for slot in range(sz.sent):
        far_all[slot] = rounded[group_row(sz, table, 0, slot)]
    for j in range((sz.groups - 1) * sz.sent):
        far_all[sz.sent + j] = far[j]

    group = table[sz.at_group]
    for i in range(sz.rows):
        parts = [rounded[table[sz.at_own + i]]]
        for k in range(sz.near):
            parts.append(near[table[sz.at_near + i * sz.near + k]])
        for k in range(sz.far):
            col = table[sz.at_far + i * sz.far + k]
            place = lax.rem(group + sz.groups - lax.div(col, sz.sent), sz.groups)
            parts.append(far_all[place * sz.sent + lax.rem(col, sz.sent)])
        left = jnp.concatenate(parts, axis=1)
        product = jnp.dot(left, blocks[i], preferred_element_type=jnp.float32)
        start = base[i, base_span] if stage < 3 else None
        v = start if stage == 0 else value[i]
        slope = rate[i : i + 1] * (v - v * v * v) - product
        if stage < 3:
            ahead = 0.5 * step_size if stage < 2 else step_size
            weight = step_size / 6.0 if stage == 0 else step_size / 3.0
            fresh = start + ahead * slope
            total_out[i] = (start if stage == 0 else total[i]) + weight * slope
        else:
            fresh = total[i] + (step_size / 6.0) * slope
        out[i] = fresh
        if not last:
            rounded_out[i] = fresh.astype(jnp.bfloat16)
    if not last:
        fill_sends(sz, table, rounded_out, member_out, group_out)


def solution(mesh):
    def per_device(state, blocks, rate, own_col, member_col, group_col, member_send, group_send):
        sz = Sizes(mesh, state, member_col, group_col, member_send, group_send)
        table = jnp.concatenate(
            [
                own_col.reshape(-1),
                member_col.reshape(-1),
                group_col.reshape(-1),
                member_send.reshape(-1),
                group_send.reshape(-1),
                lax.axis_index("group").astype(jnp.int32).reshape(1),
            ]
        )
        weights = blocks.reshape(sz.rows, -1, sz.cells)
        f32 = jax.ShapeDtypeStruct((sz.rows, sz.piece, sz.cells), jnp.float32)
        bf16 = lambda n: jax.ShapeDtypeStruct((n, sz.piece, sz.cells), jnp.bfloat16)
        sends = [bf16(sz.rows), bf16(sz.members), bf16((sz.groups - 1) * sz.sent)]
        flops = 2 * sz.rows * weights.shape[1] * sz.cells * sz.piece

        def exchange(member_out, group_out):
            far = []
            for shift in range(1, sz.groups):
                pairs = [(g, (g + shift) % sz.groups) for g in range(sz.groups)]
                sent = group_out[(shift - 1) * sz.sent : shift * sz.sent]
                far.append(lax.ppermute(sent, "group", pairs))
            far = far[0] if len(far) == 1 else jnp.concatenate(far, axis=0)
            member_out, far = lax.optimization_barrier((member_out, far))
            near = lax.all_to_all(member_out, "member", split_axis=0, concat_axis=0, tiled=True)
            return near, far

        def begin(piece):
            return pl.pallas_call(
                functools.partial(first_kernel, sz, piece),
                out_shape=sends,
                in_specs=[SMEM, VMEM],
                out_specs=[VMEM] * 3,
                compiler_params=pltpu.CompilerParams(vmem_limit_bytes=VMEM_LIMIT),
                name="begin",
            )(table, state)

        def advance(stage, last, piece, carry, near, far):
            rounded, base, value, total = carry
            whole = base.shape[1] == sz.traj
            span = pl.ds(piece * sz.piece if whole else 0, sz.piece)
            ops = [table, weights, rate, rounded, near, far]
            if stage < 3:
                ops.append(base)
            if stage > 0:
                ops += [value, total]
            outs = ([] if last else list(sends)) + [f32] + ([f32] if stage < 3 else [])
            got = pl.pallas_call(
                functools.partial(stage_kernel, sz, stage, last, span),
                out_shape=outs,
                in_specs=[SMEM] + [VMEM] * (len(ops) - 1),
                out_specs=[VMEM] * len(outs),
                scratch_shapes=[pltpu.VMEM((sz.groups * sz.sent, sz.piece, sz.cells), jnp.bfloat16)],
                compiler_params=pltpu.CompilerParams(vmem_limit_bytes=VMEM_LIMIT),
                cost_estimate=pl.CostEstimate(flops=flops, bytes_accessed=weights.size * 2, transcendentals=0),
                name="stage",
            )(*ops)
            if last:
                return got[0], None, None
            if stage < 3:
                return (got[0], base, got[3], got[4]), got[1], got[2]
            return (got[0], got[3], None, None), got[1], got[2]

        carries, outgoing = [], []
        for piece in range(PIECES):
            rounded, member_out, group_out = begin(piece)
            carries.append((rounded, state, None, None))
            outgoing.append((member_out, group_out))
        for step in range(STEPS):
            for stage in range(4):
                last = step == STEPS - 1 and stage == 3
                for piece in range(PIECES):
                    near, far = exchange(*outgoing[piece])
                    carry, member_out, group_out = advance(stage, last, piece, carries[piece], near, far)
                    carries[piece] = carry
                    outgoing[piece] = (member_out, group_out)
        return carries[0] if PIECES == 1 else jnp.concatenate(carries, axis=1)

    return jax.shard_map(
        per_device,
        mesh=mesh,
        in_specs=(
            P(("group", "member"), None, None),
            P(("group", "member"), None, None, None),
            P(("group", "member"), None),
            P(("group", "member")),
            P(("group", "member"), None),
            P(("group", "member"), None),
            P(("group", "member"), None),
            P(("group", "member"), None),
        ),
        out_specs=P(("group", "member"), None, None),
        check_vma=False,
    )
```

```python
import functools

import jax
import jax.numpy as jnp
from jax import lax
from jax.experimental import pallas as pl
from jax.experimental.pallas import tpu as pltpu
from jax.sharding import PartitionSpec as P


STEPS = 2
PIECES = 1


step_size = 0.1


VMEM = pl.BlockSpec(memory_space=pltpu.VMEM)
ANY = pl.BlockSpec(memory_space=pl.ANY)
SMEM = pl.BlockSpec(memory_space=pltpu.SMEM)


class Sizes:
    def __init__(self, mesh, state, member_col, group_col, group_send):
        self.groups = mesh.shape["group"]
        self.members = mesh.shape["member"]
        self.rows, self.traj, self.cells = state.shape
        self.near = member_col.shape[1]
        self.far = group_col.shape[1]
        self.sent = group_send.shape[1] // self.groups
        self.piece = self.traj // PIECES
        self.at_own = 0
        self.at_near = self.at_own + self.rows
        self.at_far = self.at_near + self.rows * self.near
        self.at_msend = self.at_far + self.rows * self.far
        self.at_gsend = self.at_msend + self.members
        self.at_group = self.at_gsend + self.groups * self.sent


def group_row(sz, table, shift, slot):
    target = lax.rem(table[sz.at_group] + shift, sz.groups)
    return table[sz.at_gsend + target * sz.sent + slot]


def fill_sends(sz, table, rounded, member_out, group_out):
    for p in range(sz.members):
        member_out[p] = rounded[table[sz.at_msend + p]]
    for shift in range(1, sz.groups):
        for slot in range(sz.sent):
            group_out[(shift - 1) * sz.sent + slot] = rounded[group_row(sz, table, shift, slot)]


def first_kernel(sz, piece, table, state, rounded, member_out, group_out):
    span = pl.ds(piece * sz.piece, sz.piece)
    for i in range(sz.rows):
        rounded[i] = state[i, span].astype(jnp.bfloat16)
    fill_sends(sz, table, rounded, member_out, group_out)


def stage_kernel(sz, stage, last, base_span, *refs):
    it = iter(refs)
    table, blocks, rate, rounded, near, far = (next(it) for _ in range(6))
    base = next(it) if stage < 3 else None
    value = next(it) if stage > 0 else None
    total = next(it) if stage > 0 else None
    if not last:
        rounded_out, member_out, group_out = (next(it) for _ in range(3))
    out = next(it)
    total_out = next(it) if stage < 3 else None
    far_all = next(it)

    for slot in range(sz.sent):
        far_all[slot] = rounded[group_row(sz, table, 0, slot)]
    for j in range((sz.groups - 1) * sz.sent):
        far_all[sz.sent + j] = far[j]

    group = table[sz.at_group]
    for i in range(sz.rows):
        parts = [rounded[table[sz.at_own + i]]]
        for k in range(sz.near):
            parts.append(near[table[sz.at_near + i * sz.near + k]])
        for k in range(sz.far):
            col = table[sz.at_far + i * sz.far + k]
            place = lax.rem(group + sz.groups - lax.div(col, sz.sent), sz.groups)
            parts.append(far_all[place * sz.sent + lax.rem(col, sz.sent)])
        left = jnp.concatenate(parts, axis=1)
        product = jnp.dot(left, blocks[i], preferred_element_type=jnp.float32)
        start = base[i, base_span] if stage < 3 else None
        v = start if stage == 0 else value[i]
        slope = rate[i : i + 1] * (v - v * v * v) - product
        if stage < 3:
            ahead = 0.5 * step_size if stage < 2 else step_size
            weight = step_size / 6.0 if stage == 0 else step_size / 3.0
            fresh = start + ahead * slope
            total_out[i] = (start if stage == 0 else total[i]) + weight * slope
        else:
            fresh = total[i] + (step_size / 6.0) * slope
        out[i] = fresh
        if not last:
            rounded_out[i] = fresh.astype(jnp.bfloat16)
    if not last:
        fill_sends(sz, table, rounded_out, member_out, group_out)


def solution(mesh):
    def per_device(state, blocks, rate, own_col, member_col, group_col, member_send, group_send):
        sz = Sizes(mesh, state, member_col, group_col, group_send)
        table = jnp.concatenate(
            [
                own_col.reshape(-1),
                member_col.reshape(-1),
                group_col.reshape(-1),
                member_send.reshape(-1),
                group_send.reshape(-1),
                lax.axis_index("group").astype(jnp.int32).reshape(1),
            ]
        )
        weights = blocks.reshape(sz.rows, -1, sz.cells)
        f32 = jax.ShapeDtypeStruct((sz.rows, sz.piece, sz.cells), jnp.float32)
        bf16 = lambda n: jax.ShapeDtypeStruct((n, sz.piece, sz.cells), jnp.bfloat16)
        sends = [bf16(sz.rows), bf16(sz.members), bf16((sz.groups - 1) * sz.sent)]
        limit = 16 * 2**20
        flops = 2 * sz.rows * weights.shape[1] * sz.cells * sz.piece

        def exchange(member_out, group_out):
            far = []
            for shift in range(1, sz.groups):
                pairs = [(g, (g + shift) % sz.groups) for g in range(sz.groups)]
                sent = group_out[(shift - 1) * sz.sent : shift * sz.sent]
                far.append(lax.ppermute(sent, "group", pairs))
            near = lax.all_to_all(member_out, "member", split_axis=0, concat_axis=0, tiled=True)
            near = landed(near)
            return near, far[0] if len(far) == 1 else jnp.concatenate(far, axis=0)

        def landed(near):
            return pl.pallas_call(
                lambda near, same: None,
                out_shape=near,
                in_specs=[ANY],
                out_specs=ANY,
                input_output_aliases={0: 0},
                compiler_params=pltpu.CompilerParams(vmem_limit_bytes=limit),
                name="landed",
            )(near)

        def begin(piece):
            return pl.pallas_call(
                functools.partial(first_kernel, sz, piece),
                out_shape=sends,
                in_specs=[SMEM, VMEM],
                out_specs=[VMEM] * 3,
                compiler_params=pltpu.CompilerParams(vmem_limit_bytes=limit),
                name="begin",
            )(table, state)

        def advance(stage, last, piece, carry, near, far):
            rounded, base, value, total = carry
            whole = base.shape[1] == sz.traj
            span = pl.ds(piece * sz.piece if whole else 0, sz.piece)
            ops = [table, weights, rate, rounded, near, far]
            if stage < 3:
                ops.append(base)
            if stage > 0:
                ops += [value, total]
            outs = ([] if last else list(sends)) + [f32] + ([f32] if stage < 3 else [])
            got = pl.pallas_call(
                functools.partial(stage_kernel, sz, stage, last, span),
                out_shape=outs,
                in_specs=[SMEM] + [VMEM] * (len(ops) - 1),
                out_specs=[VMEM] * len(outs),
                scratch_shapes=[pltpu.VMEM((sz.groups * sz.sent, sz.piece, sz.cells), jnp.bfloat16)],
                compiler_params=pltpu.CompilerParams(vmem_limit_bytes=limit),
                cost_estimate=pl.CostEstimate(flops=flops, bytes_accessed=weights.size * 2, transcendentals=0),
                name="stage",
            )(*ops)
            if last:
                return got[0], None, None
            if stage < 3:
                return (got[0], base, got[3], got[4]), got[1], got[2]
            return (got[0], got[3], None, None), got[1], got[2]

        carries, outgoing = [], []
        for piece in range(PIECES):
            rounded, member_out, group_out = begin(piece)
            carries.append((rounded, state, None, None))
            outgoing.append((member_out, group_out))
        for step in range(STEPS):
            for stage in range(4):
                last = step == STEPS - 1 and stage == 3
                for piece in range(PIECES):
                    near, far = exchange(*outgoing[piece])
                    carry, member_out, group_out = advance(stage, last, piece, carries[piece], near, far)
                    carries[piece] = carry
                    outgoing[piece] = (member_out, group_out)
        return carries[0] if PIECES == 1 else jnp.concatenate(carries, axis=1)

    return jax.shard_map(
        per_device,
        mesh=mesh,
        in_specs=(
            P(("group", "member"), None, None),
            P(("group", "member"), None, None, None),
            P(("group", "member"), None),
            P(("group", "member")),
            P(("group", "member"), None),
            P(("group", "member"), None),
            P(("group", "member"), None),
            P(("group", "member"), None),
        ),
        out_specs=P(("group", "member"), None, None),
        check_vma=False,
    )
```

```python
import functools

import jax
import jax.numpy as jnp
from jax import lax
from jax.experimental import pallas as pl
from jax.experimental.pallas import tpu as pltpu
from jax.sharding import PartitionSpec as P


STEPS = 2


step_size = 0.1


VMEM = pl.BlockSpec(memory_space=pltpu.VMEM)
ANY = pl.BlockSpec(memory_space=pl.ANY)
SMEM = pl.BlockSpec(memory_space=pltpu.SMEM)


class Sizes:
    def __init__(self, mesh, state, member_col, group_col, group_send):
        self.groups = mesh.shape["group"]
        self.members = mesh.shape["member"]
        self.rows, self.traj, self.cells = state.shape
        self.near = member_col.shape[1]
        self.far = group_col.shape[1]
        self.sent = group_send.shape[1] // self.groups
        self.at_own = 0
        self.at_near = self.at_own + self.rows
        self.at_far = self.at_near + self.rows * self.near
        self.at_msend = self.at_far + self.rows * self.far
        self.at_gsend = self.at_msend + self.members
        self.at_group = self.at_gsend + self.groups * self.sent


def group_row(sz, table, shift, slot):
    target = lax.rem(table[0, sz.at_group] + shift, sz.groups)
    return table[0, sz.at_gsend + target * sz.sent + slot]


def fill_sends(sz, table, rounded, member_out, group_out):
    for p in range(sz.members):
        member_out[p] = rounded[table[0, sz.at_msend + p]]
    for shift in range(1, sz.groups):
        for slot in range(sz.sent):
            group_out[(shift - 1) * sz.sent + slot] = rounded[group_row(sz, table, shift, slot)]


def first_kernel(sz, own_col, near_col, far_col, member_send, group_send, state_far, blocks_far, rate_far,
                 table_out, state, blocks, rate, rounded, member_out, group_out, table, sems):
    copies = [
        pltpu.make_async_copy(state_far, state, sems.at[0]),
        pltpu.make_async_copy(rate_far, rate, sems.at[1]),
        pltpu.make_async_copy(blocks_far, blocks, sems.at[2]),
    ]
    for copy in copies:
        copy.start()
    for i in range(sz.rows):
        table[0, sz.at_own + i] = own_col[i]
        for k in range(sz.near):
            table[0, sz.at_near + i * sz.near + k] = near_col[k, i]
        for k in range(sz.far):
            table[0, sz.at_far + i * sz.far + k] = far_col[k, i]
    for p in range(sz.members):
        table[0, sz.at_msend + p] = member_send[0, p]
    for slot in range(sz.groups * sz.sent):
        table[0, sz.at_gsend + slot] = group_send[0, slot]
    table[0, sz.at_group] = lax.axis_index("group")
    for i in range(sz.at_group + 1, table.shape[1]):
        table[0, i] = 0
    keep = pltpu.make_async_copy(table, table_out, sems.at[3])
    keep.start()
    copies[0].wait()
    for i in range(sz.rows):
        rounded[i] = state[i].astype(jnp.bfloat16)
    fill_sends(sz, table, rounded, member_out, group_out)
    keep.wait()
    copies[1].wait()
    copies[2].wait()


def stage_kernel(sz, stage, last, *refs):
    it = iter(refs)
    table, blocks, rate, rounded, near, far = (next(it) for _ in range(6))
    base = next(it) if stage < 3 else None
    value = next(it) if stage > 0 else None
    total = next(it) if stage > 0 else None
    if not last:
        rounded_out, member_out, group_out = (next(it) for _ in range(3))
    out = next(it)
    total_out = next(it) if stage < 3 else None
    far_all = next(it)

    for slot in range(sz.sent):
        far_all[slot] = rounded[group_row(sz, table, 0, slot)]
    for j in range((sz.groups - 1) * sz.sent):
        far_all[sz.sent + j] = far[j]

    group = table[0, sz.at_group]
    for i in range(sz.rows):
        parts = [rounded[table[0, sz.at_own + i]]]
        for k in range(sz.near):
            parts.append(near[table[0, sz.at_near + i * sz.near + k]])
        for k in range(sz.far):
            col = table[0, sz.at_far + i * sz.far + k]
            place = lax.rem(group + sz.groups - lax.div(col, sz.sent), sz.groups)
            parts.append(far_all[place * sz.sent + lax.rem(col, sz.sent)])
        left = jnp.concatenate(parts, axis=1)
        product = jnp.dot(left, blocks[i], preferred_element_type=jnp.float32)
        start = base[i] if stage < 3 else None
        v = start if stage == 0 else value[i]
        slope = rate[i : i + 1] * (v - v * v * v) - product
        if stage < 3:
            ahead = 0.5 * step_size if stage < 2 else step_size
            weight = step_size / 6.0 if stage == 0 else step_size / 3.0
            fresh = start + ahead * slope
            total_out[i] = (start if stage == 0 else total[i]) + weight * slope
        else:
            fresh = total[i] + (step_size / 6.0) * slope
        out[i] = fresh
        if not last:
            rounded_out[i] = fresh.astype(jnp.bfloat16)
    if not last:
        fill_sends(sz, table, rounded_out, member_out, group_out)


def solution(mesh):
    def per_device(state, blocks, rate, own_col, member_col, group_col, member_send, group_send):
        sz = Sizes(mesh, state, member_col, group_col, group_send)
        far_off = lambda x: pltpu.with_memory_space_constraint(x, pltpu.MemorySpace.HBM)
        held = lambda x: pltpu.VMEM(x.shape, x.dtype)
        weights = far_off(blocks.reshape(sz.rows, -1, sz.cells))
        entries = -(-(sz.at_group + 1) // 128) * 128
        f32 = jax.ShapeDtypeStruct((sz.rows, sz.traj, sz.cells), jnp.float32)
        bf16 = lambda n: jax.ShapeDtypeStruct((n, sz.traj, sz.cells), jnp.bfloat16)
        sends = [bf16(sz.rows), bf16(sz.members), bf16((sz.groups - 1) * sz.sent)]
        limit = 16 * 2**20
        flops = 2 * sz.rows * weights.shape[1] * sz.cells * sz.traj

        def exchange(member_out, group_out):
            far = []
            for shift in range(1, sz.groups):
                pairs = [(g, (g + shift) % sz.groups) for g in range(sz.groups)]
                sent = group_out[(shift - 1) * sz.sent : shift * sz.sent]
                far.append(lax.ppermute(sent, "group", pairs))
            near = lax.all_to_all(member_out, "member", split_axis=0, concat_axis=0, tiled=True)
            near = landed(near)
            return near, far[0] if len(far) == 1 else jnp.concatenate(far, axis=0)

        def landed(near):
            return pl.pallas_call(
                lambda near, same: None,
                out_shape=near,
                in_specs=[ANY],
                out_specs=ANY,
                input_output_aliases={0: 0},
                compiler_params=pltpu.CompilerParams(vmem_limit_bytes=limit),
                name="landed",
            )(near)

        def begin():
            tables = [own_col, member_col.T, group_col.T, member_send, group_send]
            return pl.pallas_call(
                functools.partial(first_kernel, sz),
                out_shape=[pltpu.VMEM((1, entries), jnp.int32), held(state), held(weights), held(rate), *sends],
                in_specs=[SMEM] * 5 + [ANY] * 3,
                out_specs=[VMEM] * 7,
                scratch_shapes=[pltpu.SMEM((1, entries), jnp.int32), pltpu.SemaphoreType.DMA((4,))],
                compiler_params=pltpu.CompilerParams(vmem_limit_bytes=limit),
                name="begin",
            )(*map(far_off, tables), far_off(state), weights, far_off(rate))

        def advance(stage, last, carry, near, far):
            rounded, base, value, total = carry
            ops = [table, held_weights, held_rate, rounded, near, far]
            if stage < 3:
                ops.append(base)
            if stage > 0:
                ops += [value, total]
            outs = ([] if last else list(sends)) + [f32] + ([f32] if stage < 3 else [])
            got = pl.pallas_call(
                functools.partial(stage_kernel, sz, stage, last),
                out_shape=outs,
                in_specs=[SMEM] + [VMEM] * (len(ops) - 1),
                out_specs=[VMEM] * len(outs),
                scratch_shapes=[pltpu.VMEM((sz.groups * sz.sent, sz.traj, sz.cells), jnp.bfloat16)],
                compiler_params=pltpu.CompilerParams(vmem_limit_bytes=limit),
                cost_estimate=pl.CostEstimate(flops=flops, bytes_accessed=weights.size * 2, transcendentals=0),
                name="stage",
            )(*ops)
            if last:
                return got[0], None, None
            if stage < 3:
                return (got[0], base, got[3], got[4]), got[1], got[2]
            return (got[0], got[3], None, None), got[1], got[2]

        table, base, held_weights, held_rate, rounded, member_out, group_out = begin()
        carry = (rounded, base, None, None)
        for step in range(STEPS):
            for stage in range(4):
                last = step == STEPS - 1 and stage == 3
                near, far = exchange(member_out, group_out)
                carry, member_out, group_out = advance(stage, last, carry, near, far)
        return carry

    return jax.shard_map(
        per_device,
        mesh=mesh,
        in_specs=(
            P(("group", "member"), None, None),
            P(("group", "member"), None, None, None),
            P(("group", "member"), None),
            P(("group", "member")),
            P(("group", "member"), None),
            P(("group", "member"), None),
            P(("group", "member"), None),
            P(("group", "member"), None),
        ),
        out_specs=P(("group", "member"), None, None),
        check_vma=False,
    )
```

```python
import functools

import jax
import jax.numpy as jnp
from jax import lax
from jax.experimental import pallas as pl
from jax.experimental.pallas import tpu as pltpu
from jax.sharding import PartitionSpec as P


STEPS = 2


step_size = 0.1


VMEM = pl.BlockSpec(memory_space=pltpu.VMEM)
ANY = pl.BlockSpec(memory_space=pl.ANY)
SMEM = pl.BlockSpec(memory_space=pltpu.SMEM)


class Sizes:
    def __init__(self, mesh, state, member_col, group_col, group_send):
        self.groups = mesh.shape["group"]
        self.members = mesh.shape["member"]
        self.rows, self.traj, self.cells = state.shape
        self.near = member_col.shape[1]
        self.far = group_col.shape[1]
        self.sent = group_send.shape[1] // self.groups
        self.at_own = 0
        self.at_near = self.at_own + self.rows
        self.at_far = self.at_near + self.rows * self.near
        self.at_msend = self.at_far + self.rows * self.far
        self.at_gsend = self.at_msend + self.members
        self.at_group = self.at_gsend + self.groups * self.sent


def group_row(sz, table, shift, slot):
    target = lax.rem(table[0, sz.at_group] + shift, sz.groups)
    return table[0, sz.at_gsend + target * sz.sent + slot]


def fill_sends(sz, table, rounded, member_out, group_out):
    for p in range(sz.members):
        member_out[p] = rounded[table[0, sz.at_msend + p]]
    for shift in range(1, sz.groups):
        for slot in range(sz.sent):
            group_out[(shift - 1) * sz.sent + slot] = rounded[group_row(sz, table, shift, slot)]


def first_kernel(sz, *refs):
    indices_far, (state_far, blocks_far, rate_far), refs = refs[:5], refs[5:8], refs[8:]
    (table, state, blocks, rate, rounded, member_out, group_out), refs = refs[:7], refs[7:]
    indices, sems = refs[:5], refs[5]
    own_col, near_col, far_col, member_send, group_send = indices
    copies = [
        pltpu.make_async_copy(source, target, sems.at[n])
        for n, (source, target) in enumerate(
            zip((state_far, rate_far, *indices_far, blocks_far), (state, rate, *indices, blocks))
        )
    ]
    for copy in copies:
        copy.start()
    for copy in copies[2:7]:
        copy.wait()
    for i in range(sz.rows):
        table[0, sz.at_own + i] = own_col[i]
        for k in range(sz.near):
            table[0, sz.at_near + i * sz.near + k] = near_col[k, i]
        for k in range(sz.far):
            table[0, sz.at_far + i * sz.far + k] = far_col[k, i]
    for p in range(sz.members):
        table[0, sz.at_msend + p] = member_send[0, p]
    for slot in range(sz.groups * sz.sent):
        table[0, sz.at_gsend + slot] = group_send[0, slot]
    table[0, sz.at_group] = lax.axis_index("group")
    for i in range(sz.at_group + 1, table.shape[1]):
        table[0, i] = 0
    copies[0].wait()
    for i in range(sz.rows):
        rounded[i] = state[i].astype(jnp.bfloat16)
    fill_sends(sz, table, rounded, member_out, group_out)
    copies[1].wait()
    copies[7].wait()


def stage_kernel(sz, stage, last, *refs):
    it = iter(refs)
    table, blocks, rate, rounded, near, far = (next(it) for _ in range(6))
    base = next(it) if stage < 3 else None
    value = next(it) if stage > 0 else None
    total = next(it) if stage > 0 else None
    if not last:
        rounded_out, member_out, group_out = (next(it) for _ in range(3))
    out = next(it)
    total_out = next(it) if stage < 3 else None
    far_all = next(it)

    for slot in range(sz.sent):
        far_all[slot] = rounded[group_row(sz, table, 0, slot)]
    for j in range((sz.groups - 1) * sz.sent):
        far_all[sz.sent + j] = far[j]

    group = table[0, sz.at_group]
    for i in range(sz.rows):
        parts = [rounded[table[0, sz.at_own + i]]]
        for k in range(sz.near):
            parts.append(near[table[0, sz.at_near + i * sz.near + k]])
        for k in range(sz.far):
            col = table[0, sz.at_far + i * sz.far + k]
            place = lax.rem(group + sz.groups - lax.div(col, sz.sent), sz.groups)
            parts.append(far_all[place * sz.sent + lax.rem(col, sz.sent)])
        left = jnp.concatenate(parts, axis=1)
        product = jnp.dot(left, blocks[i], preferred_element_type=jnp.float32)
        start = base[i] if stage < 3 else None
        v = start if stage == 0 else value[i]
        slope = rate[i : i + 1] * (v - v * v * v) - product
        if stage < 3:
            ahead = 0.5 * step_size if stage < 2 else step_size
            weight = step_size / 6.0 if stage == 0 else step_size / 3.0
            fresh = start + ahead * slope
            total_out[i] = (start if stage == 0 else total[i]) + weight * slope
        else:
            fresh = total[i] + (step_size / 6.0) * slope
        out[i] = fresh
        if not last:
            rounded_out[i] = fresh.astype(jnp.bfloat16)
    if not last:
        fill_sends(sz, table, rounded_out, member_out, group_out)


def solution(mesh):
    def per_device(state, blocks, rate, own_col, member_col, group_col, member_send, group_send):
        sz = Sizes(mesh, state, member_col, group_col, group_send)
        far_off = lambda x: pltpu.with_memory_space_constraint(x, pltpu.MemorySpace.HBM)
        held = lambda x: pltpu.VMEM(x.shape, x.dtype)
        weights = far_off(blocks.reshape(sz.rows, -1, sz.cells))
        entries = -(-(sz.at_group + 1) // 128) * 128
        f32 = jax.ShapeDtypeStruct((sz.rows, sz.traj, sz.cells), jnp.float32)
        bf16 = lambda n: jax.ShapeDtypeStruct((n, sz.traj, sz.cells), jnp.bfloat16)
        sends = [bf16(sz.rows), bf16(sz.members), bf16((sz.groups - 1) * sz.sent)]
        limit = 16 * 2**20
        flops = 2 * sz.rows * weights.shape[1] * sz.cells * sz.traj

        def exchange(member_out, group_out):
            far = []
            for shift in range(1, sz.groups):
                pairs = [(g, (g + shift) % sz.groups) for g in range(sz.groups)]
                sent = group_out[(shift - 1) * sz.sent : shift * sz.sent]
                far.append(lax.ppermute(sent, "group", pairs))
            near = lax.all_to_all(member_out, "member", split_axis=0, concat_axis=0, tiled=True)
            near = landed(near)
            return near, far[0] if len(far) == 1 else jnp.concatenate(far, axis=0)

        def landed(near):
            return pl.pallas_call(
                lambda near, same: None,
                out_shape=near,
                in_specs=[ANY],
                out_specs=ANY,
                input_output_aliases={0: 0},
                compiler_params=pltpu.CompilerParams(vmem_limit_bytes=limit),
                name="landed",
            )(near)

        def begin():
            tables = [own_col, member_col.T, group_col.T, member_send, group_send]
            return pl.pallas_call(
                functools.partial(first_kernel, sz),
                out_shape=[pltpu.SMEM((1, entries), jnp.int32), held(state), held(weights), held(rate), *sends],
                in_specs=[ANY] * 8,
                out_specs=[SMEM] + [VMEM] * 6,
                scratch_shapes=[pltpu.SMEM(x.shape, x.dtype) for x in tables] + [pltpu.SemaphoreType.DMA((8,))],
                compiler_params=pltpu.CompilerParams(vmem_limit_bytes=limit),
                name="begin",
            )(*map(far_off, tables), far_off(state), weights, far_off(rate))

        def advance(stage, last, carry, near, far):
            rounded, base, value, total = carry
            ops = [table, held_weights, held_rate, rounded, near, far]
            if stage < 3:
                ops.append(base)
            if stage > 0:
                ops += [value, total]
            outs = ([] if last else list(sends)) + [f32] + ([f32] if stage < 3 else [])
            got = pl.pallas_call(
                functools.partial(stage_kernel, sz, stage, last),
                out_shape=outs,
                in_specs=[SMEM] + [VMEM] * (len(ops) - 1),
                out_specs=[VMEM] * len(outs),
                scratch_shapes=[pltpu.VMEM((sz.groups * sz.sent, sz.traj, sz.cells), jnp.bfloat16)],
                compiler_params=pltpu.CompilerParams(vmem_limit_bytes=limit),
                cost_estimate=pl.CostEstimate(flops=flops, bytes_accessed=weights.size * 2, transcendentals=0),
                name="stage",
            )(*ops)
            if last:
                return got[0], None, None
            if stage < 3:
                return (got[0], base, got[3], got[4]), got[1], got[2]
            return (got[0], got[3], None, None), got[1], got[2]

        table, base, held_weights, held_rate, rounded, member_out, group_out = begin()
        carry = (rounded, base, None, None)
        for step in range(STEPS):
            for stage in range(4):
                last = step == STEPS - 1 and stage == 3
                near, far = exchange(member_out, group_out)
                carry, member_out, group_out = advance(stage, last, carry, near, far)
        return carry

    return jax.shard_map(
        per_device,
        mesh=mesh,
        in_specs=(
            P(("group", "member"), None, None),
            P(("group", "member"), None, None, None),
            P(("group", "member"), None),
            P(("group", "member")),
            P(("group", "member"), None),
            P(("group", "member"), None),
            P(("group", "member"), None),
            P(("group", "member"), None),
        ),
        out_specs=P(("group", "member"), None, None),
        check_vma=False,
    )
```

```python
import functools

import jax
import jax.numpy as jnp
from jax import lax
from jax.experimental import pallas as pl
from jax.experimental.pallas import tpu as pltpu
from jax.sharding import PartitionSpec as P


STEPS = 2


step_size = 0.1


VMEM = pl.BlockSpec(memory_space=pltpu.VMEM)
ANY = pl.BlockSpec(memory_space=pl.ANY)
SMEM = pl.BlockSpec(memory_space=pltpu.SMEM)


class Sizes:
    def __init__(self, mesh, state, member_col, group_col, group_send):
        self.groups = mesh.shape["group"]
        self.members = mesh.shape["member"]
        self.rows, self.traj, self.cells = state.shape
        self.near = member_col.shape[1]
        self.far = group_col.shape[1]
        self.sent = group_send.shape[1] // self.groups
        self.at_own = 0
        self.at_near = self.at_own + self.rows
        self.at_far = self.at_near + self.rows * self.near
        self.at_msend = self.at_far + self.rows * self.far
        self.at_gsend = self.at_msend + self.members
        self.at_group = self.at_gsend + self.groups * self.sent


def group_row(sz, table, shift, slot):
    target = lax.rem(table[0, sz.at_group] + shift, sz.groups)
    return table[0, sz.at_gsend + target * sz.sent + slot]


def fill_sends(sz, table, rounded, member_out, group_out):
    for p in range(sz.members):
        member_out[p] = rounded[table[0, sz.at_msend + p]]
    for shift in range(1, sz.groups):
        for slot in range(sz.sent):
            group_out[(shift - 1) * sz.sent + slot] = rounded[group_row(sz, table, shift, slot)]


def first_kernel(sz, *refs):
    indices_far, (state_far, rate_far), refs = refs[:5], refs[5:7], refs[7:]
    (table, state, rate, rounded, member_out, group_out), refs = refs[:6], refs[6:]
    indices, sems = refs[:5], refs[5]
    own_col, near_col, far_col, member_send, group_send = indices
    copies = [
        pltpu.make_async_copy(source, target, sems.at[n])
        for n, (source, target) in enumerate(
            zip((state_far, rate_far, *indices_far), (state, rate, *indices))
        )
    ]
    for copy in copies:
        copy.start()
    for copy in copies[2:7]:
        copy.wait()
    for i in range(sz.rows):
        table[0, sz.at_own + i] = own_col[i]
        for k in range(sz.near):
            table[0, sz.at_near + i * sz.near + k] = near_col[k, i]
        for k in range(sz.far):
            table[0, sz.at_far + i * sz.far + k] = far_col[k, i]
    for p in range(sz.members):
        table[0, sz.at_msend + p] = member_send[0, p]
    for slot in range(sz.groups * sz.sent):
        table[0, sz.at_gsend + slot] = group_send[0, slot]
    table[0, sz.at_group] = lax.axis_index("group")
    for i in range(sz.at_group + 1, table.shape[1]):
        table[0, i] = 0
    copies[0].wait()
    for i in range(sz.rows):
        rounded[i] = state[i].astype(jnp.bfloat16)
    fill_sends(sz, table, rounded, member_out, group_out)
    copies[1].wait()


def stage_kernel(sz, stage, last, *refs):
    it = iter(refs)
    table, blocks, rate, rounded, near, far = (next(it) for _ in range(6))
    base = next(it) if stage < 3 else None
    value = next(it) if stage > 0 else None
    total = next(it) if stage > 0 else None
    if not last:
        rounded_out, member_out, group_out = (next(it) for _ in range(3))
    out = next(it)
    total_out = next(it) if stage < 3 else None
    far_all = next(it)

    for slot in range(sz.sent):
        far_all[slot] = rounded[group_row(sz, table, 0, slot)]
    for j in range((sz.groups - 1) * sz.sent):
        far_all[sz.sent + j] = far[j]

    group = table[0, sz.at_group]
    for i in range(sz.rows):
        parts = [rounded[table[0, sz.at_own + i]]]
        for k in range(sz.near):
            parts.append(near[table[0, sz.at_near + i * sz.near + k]])
        for k in range(sz.far):
            col = table[0, sz.at_far + i * sz.far + k]
            place = lax.rem(group + sz.groups - lax.div(col, sz.sent), sz.groups)
            parts.append(far_all[place * sz.sent + lax.rem(col, sz.sent)])
        left = jnp.concatenate(parts, axis=1)
        product = jnp.dot(left, blocks[i], preferred_element_type=jnp.float32)
        start = base[i] if stage < 3 else None
        v = start if stage == 0 else value[i]
        slope = rate[i : i + 1] * (v - v * v * v) - product
        if stage < 3:
            ahead = 0.5 * step_size if stage < 2 else step_size
            weight = step_size / 6.0 if stage == 0 else step_size / 3.0
            fresh = start + ahead * slope
            total_out[i] = (start if stage == 0 else total[i]) + weight * slope
        else:
            fresh = total[i] + (step_size / 6.0) * slope
        out[i] = fresh
        if not last:
            rounded_out[i] = fresh.astype(jnp.bfloat16)
    if not last:
        fill_sends(sz, table, rounded_out, member_out, group_out)


def solution(mesh):
    def per_device(state, blocks, rate, own_col, member_col, group_col, member_send, group_send):
        sz = Sizes(mesh, state, member_col, group_col, group_send)
        far_off = lambda x: pltpu.with_memory_space_constraint(x, pltpu.MemorySpace.HBM)
        held = lambda x: pltpu.VMEM(x.shape, x.dtype)
        weights = blocks.reshape(sz.rows, -1, sz.cells)
        entries = -(-(sz.at_group + 1) // 128) * 128
        f32 = jax.ShapeDtypeStruct((sz.rows, sz.traj, sz.cells), jnp.float32)
        bf16 = lambda n: jax.ShapeDtypeStruct((n, sz.traj, sz.cells), jnp.bfloat16)
        sends = [bf16(sz.rows), bf16(sz.members), bf16((sz.groups - 1) * sz.sent)]
        limit = 16 * 2**20
        flops = 2 * sz.rows * weights.shape[1] * sz.cells * sz.traj

        def exchange(member_out, group_out):
            far = []
            for shift in range(1, sz.groups):
                pairs = [(g, (g + shift) % sz.groups) for g in range(sz.groups)]
                sent = group_out[(shift - 1) * sz.sent : shift * sz.sent]
                far.append(lax.ppermute(sent, "group", pairs))
            near = lax.all_to_all(member_out, "member", split_axis=0, concat_axis=0, tiled=True)
            near = landed(near)
            return near, far[0] if len(far) == 1 else jnp.concatenate(far, axis=0)

        def landed(near):
            return pl.pallas_call(
                lambda near, same: None,
                out_shape=near,
                in_specs=[ANY],
                out_specs=ANY,
                input_output_aliases={0: 0},
                compiler_params=pltpu.CompilerParams(vmem_limit_bytes=limit),
                name="landed",
            )(near)

        def begin():
            tables = [own_col, member_col.T, group_col.T, member_send, group_send]
            return pl.pallas_call(
                functools.partial(first_kernel, sz),
                out_shape=[pltpu.SMEM((1, entries), jnp.int32), held(state), held(rate), *sends],
                in_specs=[ANY] * 7,
                out_specs=[SMEM] + [VMEM] * 5,
                scratch_shapes=[pltpu.SMEM(x.shape, x.dtype) for x in tables] + [pltpu.SemaphoreType.DMA((7,))],
                compiler_params=pltpu.CompilerParams(vmem_limit_bytes=limit),
                cost_estimate=pl.CostEstimate(flops=4 * flops, bytes_accessed=state.size * 4, transcendentals=0),
                name="begin",
            )(*map(far_off, tables), far_off(state), far_off(rate))

        def advance(stage, last, carry, near, far):
            rounded, base, value, total = carry
            ops = [table, weights, held_rate, rounded, near, far]
            if stage < 3:
                ops.append(base)
            if stage > 0:
                ops += [value, total]
            outs = ([] if last else list(sends)) + [f32] + ([f32] if stage < 3 else [])
            got = pl.pallas_call(
                functools.partial(stage_kernel, sz, stage, last),
                out_shape=outs,
                in_specs=[SMEM] + [VMEM] * (len(ops) - 1),
                out_specs=[VMEM] * len(outs),
                scratch_shapes=[pltpu.VMEM((sz.groups * sz.sent, sz.traj, sz.cells), jnp.bfloat16)],
                compiler_params=pltpu.CompilerParams(vmem_limit_bytes=limit),
                cost_estimate=pl.CostEstimate(flops=flops, bytes_accessed=weights.size * 2, transcendentals=0),
                name="stage",
            )(*ops)
            if last:
                return got[0], None, None
            if stage < 3:
                return (got[0], base, got[3], got[4]), got[1], got[2]
            return (got[0], got[3], None, None), got[1], got[2]

        table, base, held_rate, rounded, member_out, group_out = begin()
        carry = (rounded, base, None, None)
        for step in range(STEPS):
            for stage in range(4):
                last = step == STEPS - 1 and stage == 3
                near, far = exchange(member_out, group_out)
                carry, member_out, group_out = advance(stage, last, carry, near, far)
        return carry

    return jax.shard_map(
        per_device,
        mesh=mesh,
        in_specs=(
            P(("group", "member"), None, None),
            P(("group", "member"), None, None, None),
            P(("group", "member"), None),
            P(("group", "member")),
            P(("group", "member"), None),
            P(("group", "member"), None),
            P(("group", "member"), None),
            P(("group", "member"), None),
        ),
        out_specs=P(("group", "member"), None, None),
        check_vma=False,
    )
```

```python
import functools

import jax
import jax.numpy as jnp
from jax import lax
from jax.experimental import pallas as pl
from jax.experimental.pallas import tpu as pltpu
from jax.sharding import PartitionSpec as P


STEPS = 2


step_size = 0.1


VMEM = pl.BlockSpec(memory_space=pltpu.VMEM)
ANY = pl.BlockSpec(memory_space=pl.ANY)
SMEM = pl.BlockSpec(memory_space=pltpu.SMEM)


class Sizes:
    def __init__(self, mesh, state, member_col, group_col, group_send):
        self.groups = mesh.shape["group"]
        self.members = mesh.shape["member"]
        self.rows, self.traj, self.cells = state.shape
        self.burst = 4 if self.rows % 4 == 0 else 1
        self.near = member_col.shape[1]
        self.far = group_col.shape[1]
        self.sent = group_send.shape[1] // self.groups
        self.at_own = 0
        self.at_near = self.at_own + self.rows
        self.at_far = self.at_near + self.rows * self.near
        self.at_msend = self.at_far + self.rows * self.far
        self.at_gsend = self.at_msend + self.members
        self.at_group = self.at_gsend + self.groups * self.sent


def group_row(sz, table, shift, slot):
    target = lax.rem(table[0, sz.at_group] + shift, sz.groups)
    return table[0, sz.at_gsend + target * sz.sent + slot]


def fill_sends(sz, table, rounded, member_out, group_out):
    for p in range(sz.members):
        member_out[p] = rounded[table[0, sz.at_msend + p]]
    for shift in range(1, sz.groups):
        for slot in range(sz.sent):
            group_out[(shift - 1) * sz.sent + slot] = rounded[group_row(sz, table, shift, slot)]


def first_kernel(sz, *refs):
    indices_far, (state_far, rate_far), refs = refs[:5], refs[5:7], refs[7:]
    (table, state, rate, rounded, member_out, group_out), refs = refs[:6], refs[6:]
    indices, sems = refs[:5], refs[5]
    own_col, near_col, far_col, member_send, group_send = indices
    copies = [
        pltpu.make_async_copy(source, target, sems.at[n])
        for n, (source, target) in enumerate(
            zip((state_far, rate_far, *indices_far), (state, rate, *indices))
        )
    ]
    for copy in copies:
        copy.start()
    for copy in copies[2:7]:
        copy.wait()
    for i in range(sz.rows):
        table[0, sz.at_own + i] = own_col[i]
        for k in range(sz.near):
            table[0, sz.at_near + i * sz.near + k] = near_col[k, i]
        for k in range(sz.far):
            table[0, sz.at_far + i * sz.far + k] = far_col[k, i]
    for p in range(sz.members):
        table[0, sz.at_msend + p] = member_send[0, p]
    for slot in range(sz.groups * sz.sent):
        table[0, sz.at_gsend + slot] = group_send[0, slot]
    table[0, sz.at_group] = lax.axis_index("group")
    for i in range(sz.at_group + 1, table.shape[1]):
        table[0, i] = 0
    copies[0].wait()
    for i in range(sz.rows):
        rounded[i] = state[i].astype(jnp.bfloat16)
    fill_sends(sz, table, rounded, member_out, group_out)
    copies[1].wait()


def stage_kernel(sz, stage, last, *refs):
    it = iter(refs)
    table, blocks, rate, rounded, near, far = (next(it) for _ in range(6))
    base = next(it) if stage < 3 else None
    value = next(it) if stage > 0 else None
    total = next(it) if stage > 0 else None
    if not last:
        rounded_out, member_out, group_out = (next(it) for _ in range(3))
    out = next(it)
    total_out = next(it) if stage < 3 else None
    far_all = next(it)
    if last:
        whole, out, sems = out, *it
    finals = []

    for slot in range(sz.sent):
        far_all[slot] = rounded[group_row(sz, table, 0, slot)]
    for j in range((sz.groups - 1) * sz.sent):
        far_all[sz.sent + j] = far[j]

    group = table[0, sz.at_group]
    for i in range(sz.rows):
        parts = [rounded[table[0, sz.at_own + i]]]
        for k in range(sz.near):
            parts.append(near[table[0, sz.at_near + i * sz.near + k]])
        for k in range(sz.far):
            col = table[0, sz.at_far + i * sz.far + k]
            place = lax.rem(group + sz.groups - lax.div(col, sz.sent), sz.groups)
            parts.append(far_all[place * sz.sent + lax.rem(col, sz.sent)])
        left = jnp.concatenate(parts, axis=1)
        product = jnp.dot(left, blocks[i], preferred_element_type=jnp.float32)
        start = base[i] if stage < 3 else None
        v = start if stage == 0 else value[i]
        slope = rate[i : i + 1] * (v - v * v * v) - product
        if stage < 3:
            ahead = 0.5 * step_size if stage < 2 else step_size
            weight = step_size / 6.0 if stage == 0 else step_size / 3.0
            fresh = start + ahead * slope
            total_out[i] = (start if stage == 0 else total[i]) + weight * slope
        else:
            fresh = total[i] + (step_size / 6.0) * slope
        out[i] = fresh
        if last and (i + 1) % sz.burst == 0:
            done = pl.ds(i + 1 - sz.burst, sz.burst)
            finals.append(pltpu.make_async_copy(out.at[done], whole.at[done], sems.at[i // sz.burst]))
            finals[-1].start()
        if not last:
            rounded_out[i] = fresh.astype(jnp.bfloat16)
    if not last:
        fill_sends(sz, table, rounded_out, member_out, group_out)
    for copy in finals:
        copy.wait()


def solution(mesh):
    def per_device(state, blocks, rate, own_col, member_col, group_col, member_send, group_send):
        sz = Sizes(mesh, state, member_col, group_col, group_send)
        far_off = lambda x: pltpu.with_memory_space_constraint(x, pltpu.MemorySpace.HBM)
        held = lambda x: pltpu.VMEM(x.shape, x.dtype)
        weights = blocks.reshape(sz.rows, -1, sz.cells)
        entries = -(-(sz.at_group + 1) // 128) * 128
        f32 = jax.ShapeDtypeStruct((sz.rows, sz.traj, sz.cells), jnp.float32)
        bf16 = lambda n: jax.ShapeDtypeStruct((n, sz.traj, sz.cells), jnp.bfloat16)
        sends = [bf16(sz.rows), bf16(sz.members), bf16((sz.groups - 1) * sz.sent)]
        limit = 16 * 2**20
        flops = 2 * sz.rows * weights.shape[1] * sz.cells * sz.traj

        def exchange(member_out, group_out):
            far = []
            for shift in range(1, sz.groups):
                pairs = [(g, (g + shift) % sz.groups) for g in range(sz.groups)]
                sent = group_out[(shift - 1) * sz.sent : shift * sz.sent]
                far.append(lax.ppermute(sent, "group", pairs))
            near = lax.all_to_all(member_out, "member", split_axis=0, concat_axis=0, tiled=True)
            near = landed(near)
            return near, far[0] if len(far) == 1 else jnp.concatenate(far, axis=0)

        def landed(near):
            return pl.pallas_call(
                lambda near, same: None,
                out_shape=near,
                in_specs=[ANY],
                out_specs=ANY,
                input_output_aliases={0: 0},
                compiler_params=pltpu.CompilerParams(vmem_limit_bytes=limit),
                name="landed",
            )(near)

        def begin():
            tables = [own_col, member_col.T, group_col.T, member_send, group_send]
            return pl.pallas_call(
                functools.partial(first_kernel, sz),
                out_shape=[pltpu.SMEM((1, entries), jnp.int32), held(state), held(rate), *sends],
                in_specs=[ANY] * 7,
                out_specs=[SMEM] + [VMEM] * 5,
                scratch_shapes=[pltpu.SMEM(x.shape, x.dtype) for x in tables] + [pltpu.SemaphoreType.DMA((7,))],
                compiler_params=pltpu.CompilerParams(vmem_limit_bytes=limit),
                cost_estimate=pl.CostEstimate(flops=4 * flops, bytes_accessed=state.size * 4, transcendentals=0),
                name="begin",
            )(*map(far_off, tables), far_off(state), far_off(rate))

        def advance(stage, last, carry, near, far):
            rounded, base, value, total = carry
            ops = [table, weights, held_rate, rounded, near, far]
            if stage < 3:
                ops.append(base)
            if stage > 0:
                ops += [value, total]
            outs = [state] if last else [*sends, f32] + ([f32] if stage < 3 else [])
            outs = [jax.ShapeDtypeStruct(x.shape, x.dtype) if last else x for x in outs]
            extra = [pltpu.VMEM(state.shape, state.dtype), pltpu.SemaphoreType.DMA((sz.rows // sz.burst,))] if last else []
            got = pl.pallas_call(
                functools.partial(stage_kernel, sz, stage, last),
                out_shape=outs,
                in_specs=[SMEM] + [VMEM] * (len(ops) - 1),
                out_specs=[ANY if last else VMEM] * len(outs),
                scratch_shapes=[pltpu.VMEM((sz.groups * sz.sent, sz.traj, sz.cells), jnp.bfloat16), *extra],
                compiler_params=pltpu.CompilerParams(vmem_limit_bytes=limit),
                cost_estimate=pl.CostEstimate(flops=flops, bytes_accessed=weights.size * 2, transcendentals=0),
                name="stage",
            )(*ops)
            if last:
                return got[0], None, None
            if stage < 3:
                return (got[0], base, got[3], got[4]), got[1], got[2]
            return (got[0], got[3], None, None), got[1], got[2]

        table, base, held_rate, rounded, member_out, group_out = begin()
        carry = (rounded, base, None, None)
        for step in range(STEPS):
            for stage in range(4):
                last = step == STEPS - 1 and stage == 3
                near, far = exchange(member_out, group_out)
                carry, member_out, group_out = advance(stage, last, carry, near, far)
        return carry

    return jax.shard_map(
        per_device,
        mesh=mesh,
        in_specs=(
            P(("group", "member"), None, None),
            P(("group", "member"), None, None, None),
            P(("group", "member"), None),
            P(("group", "member")),
            P(("group", "member"), None),
            P(("group", "member"), None),
            P(("group", "member"), None),
            P(("group", "member"), None),
        ),
        out_specs=P(("group", "member"), None, None),
        check_vma=False,
    )
```
